32 devices in a mesh: gx: 4 (over y, core), gy: 8 (over z, x).
Axes of the slice: x: 2, y: 2, z: 4, core: 2. Of those that a mesh axis runs over, the one named last changes fastest.
Arguments:
- old_master: float32 [32, 128, 1536], P('gx', 'gy'), may hold values from -3 to 3
- old_first: float32 [32, 128, 1536], P('gx', 'gy'), may hold values from -3 to 3
- old_second: float32 [32, 128, 1536], P('gx', 'gy'), may hold values from 0.01 to 1
- new_grad: bfloat16 [32, 128, 1536], P(('gx', 'gy')), may hold values from -3072 to 3072
- counts: int32 [32, 32], P(None, ('gx', 'gy')), may hold values from 1 to 72, as said below
- old_owner: int32 [32], replicated, may hold values from 0 to 31, each once
- new_owner: int32 [32], replicated, may hold values from 0 to 31, each once
Outputs:
- new_master: float32 [32, 128, 1536], P(('gx', 'gy'))
- new_first: float32 [32, 128, 1536], P(('gx', 'gy'))
- new_second: float32 [32, 128, 1536], P(('gx', 'gy'))
The draws below stay inside these ranges and needn't reach their ends.
Inputs may be any that keep to these rules, and one draw needn't show every extreme that they name: `old_owner`: every number of 0 to 31 appears once. `new_owner`: every number of 0 to 31 appears once. `counts`: every device routed at least one token to every expert.
All inputs are finite; a program needn't handle non-finite values.
Results may differ from the reference program's by a relative error of at most 0.0003.
Values sent between devices are 32-bit elements; how exact they have to be, the bound alone decides.
A program may use at most 64 MiB of HBM per device.

```python
import math
import jax
import jax.numpy as jnp
from jax import lax

FF = 1536
ROWS = 128
EXPERTS = 32
RANKS = 32


def draw_counts(key, part):
    key_tokens = jax.random.fold_in(key, 11)
    key_skew = jax.random.fold_in(key, 23)
    columns = jnp.arange(RANKS, dtype=jnp.int32)
    ceiling = 6 + 12 * columns // max(RANKS - 1, 1)
    factor = 1 + jax.random.randint(key_skew, (EXPERTS,), 0, 4)
    base = 1 + jax.random.randint(key_tokens, (EXPERTS, RANKS), 0, ceiling[None, :])
    return (base * factor[:, None]).astype(jnp.int32)


def block_scale(stream_key, dims, pieces, low, top_value):
    def one(axis_at, parts):
        heights = jax.random.uniform(jax.random.fold_in(jax.random.fold_in(stream_key, 6), axis_at), (parts,), jnp.float32, low / len(pieces), top_value / len(pieces))
        return jnp.repeat(jnp.exp(heights), dims[axis_at] // parts).reshape((-1,) + (1,) * (len(dims) - axis_at - 1))

    level = one(*pieces[0])
    for cut in pieces[1:]:
        level = level * one(*cut)
    return level


def bell_draw(key, extent, scale, limit, cuts=(), kind=jnp.bfloat16):
    values = jax.random.normal(key, extent, jnp.float32) * scale
    if len(cuts) > 0:
        values = block_scale(key, extent, cuts, -0.22, 0.18) * values
    return jnp.clip(values, min=-limit, max=limit).astype(kind)


def setup_inputs(seed: int = 0) -> dict:
    seeds = jax.random.split(jax.random.key(seed), 8)
    old_master = bell_draw(seeds[0], (EXPERTS, ROWS, FF), 0.5, 3.0, ((0, 4), (1, 8)), jnp.float32)
    old_first = bell_draw(seeds[1], (EXPERTS, ROWS, FF), 0.5, 3.0, ((0, 4), (1, 8)), jnp.float32)
    old_second = jnp.clip(jnp.exp(math.log(1.0) - 4.6051702 * jax.random.uniform(seeds[2], (EXPERTS, ROWS, FF), jnp.float32) ** block_scale(seeds[2], (EXPERTS, ROWS, FF), ((0, 4), (1, 8)), -0.2, 0.2)), 0.01, 1.0)
    new_grad = bell_draw(seeds[3], (EXPERTS, ROWS, FF), (16 * EXPERTS), 3072.0, ((0, 32),))
    counts = draw_counts(jax.random.fold_in(seeds[7], 71), 0)
    old_owner = jax.random.permutation(seeds[5], EXPERTS).astype(jnp.int32)
    new_owner = jax.random.permutation(seeds[6], EXPERTS).astype(jnp.int32)
    return {"old_master": old_master, "old_first": old_first, "old_second": old_second, "new_grad": new_grad, "counts": counts, "old_owner": old_owner, "new_owner": new_owner}


first_correction = 1.0 - 0.9 ** 10
second_correction = 1.0 - 0.999 ** 10

def adam_step(master, first, second, grad, slot_count):
    scaled = grad.astype(jnp.float32) / slot_count
    new_first = 0.9 * first + 0.1 * scaled
    new_second = 0.999 * second + 0.001 * scaled * scaled
    step_dir = new_first / first_correction / (jnp.sqrt(new_second / second_correction) + 1e-08)
    new_master = master - 0.01 * (step_dir + 0.1 * master)
    return (new_master, new_first, new_second)

def reference(old_master, old_first, old_second, new_grad, counts, old_owner, new_owner):
    slots = jnp.arange(EXPERTS, dtype=jnp.int32)
    onehot = new_owner[:, None] == slots[None, :]
    source = lax.optimization_barrier(jnp.sum(jnp.where(onehot, old_owner[:, None], 0), axis=0)).astype(jnp.int32)
    totals = lax.optimization_barrier(jnp.sum(counts.astype(jnp.float32), axis=1))
    slot_count = lax.optimization_barrier(jnp.sum(jnp.where(onehot, totals[:, None], jnp.float32(0.0)), axis=0))
    master = jnp.take(old_master, source, axis=0)
    first = jnp.take(old_first, source, axis=0)
    second = jnp.take(old_second, source, axis=0)
    return adam_step(master, first, second, new_grad, slot_count[:, None, None])
```

```python
import functools

import jax
import jax.numpy as jnp
from jax import lax
from jax.experimental import pallas as pl
from jax.experimental.pallas import tpu as pltpu
from jax.sharding import PartitionSpec as P

first_correction = 1.0 - 0.9**10
second_correction = 1.0 - 0.999**10
MESH = pl.DeviceIdType.MESH
LANES = 128
SUBLANES = 8
SUBCHUNKS = 2


def adam_step(master, first, second, grad, slot_count):
    scaled = grad.astype(jnp.float32) / slot_count
    new_first = 0.9 * first + 0.1 * scaled
    new_second = 0.999 * second + 0.001 * scaled * scaled
    step_dir = new_first / first_correction / (jnp.sqrt(new_second / second_correction) + 1e-08)
    new_master = master - 0.01 * (step_dir + 0.1 * master)
    return (new_master, new_first, new_second)


def reorder(block, groups_x, groups_y):
    total_rows = block.shape[1]
    piece = total_rows // (groups_x * groups_y)
    shaped = block.reshape(1, groups_x, groups_y, piece, block.shape[2])
    return shaped.transpose(0, 2, 1, 3, 4).reshape(1, total_rows, block.shape[2])


def plain_body(old_master, old_first, old_second, new_grad, counts, old_owner, new_owner):
    experts = old_owner.shape[0]
    groups_x = lax.axis_size("gx")
    groups_y = lax.axis_size("gy")
    my_slot = lax.axis_index("gx") * groups_y + lax.axis_index("gy")
    slots = jnp.arange(experts, dtype=jnp.int32)
    onehot = new_owner[:, None] == slots[None, :]
    source = jnp.sum(jnp.where(onehot, old_owner[:, None], 0), axis=0)
    local_counts = counts[:, 0].astype(jnp.float32)
    by_rows = tuple(
        lax.all_to_all(state, "gx", split_axis=1, concat_axis=0, tiled=True)
        for state in (old_master, old_first, old_second)
    )
    permuted = tuple((jnp.take(state, source, axis=0) for state in by_rows))
    landed = lax.all_to_all(permuted, ("gx", "gy"), split_axis=0, concat_axis=1, tiled=True)
    arrived = tuple((reorder(state, groups_x, groups_y) for state in landed))
    totals = lax.psum(local_counts, ("gx", "gy"))
    slot_count = jnp.sum(jnp.where(new_owner == my_slot, totals, jnp.float32(0.0)))
    return adam_step(arrived[0], arrived[1], arrived[2], new_grad, slot_count)


def rehome_kernel(dims, old_owner, new_owner, owner_row, count_row, old_m, old_f, old_s, *rest):
    groups_x, groups_y, experts, held, rows, tiles, width, chunks = dims
    outs, count_out = rest[:3], rest[3]
    by_rows = rest[4 : 4 + chunks]
    staged = rest[4 + chunks : 4 + 2 * chunks]
    (source, all_counts, local_sem, send1, recv1, send2, recv2, send_c, recv_c) = rest[4 + 2 * chunks :]
    olds = (old_m, old_f, old_s)
    devices = groups_x * groups_y
    per_state = chunks // 3
    splits = groups_x // tiles
    span = per_state * width
    gx = lax.axis_index("gx")
    gy = lax.axis_index("gy")
    me = gx * groups_y + gy

    def peer(i):
        at = i // groups_x
        sign = 1 - 2 * (at % 2)
        off = groups_y // 2 + sign * ((at + 1) // 2)
        px = (gx + i % groups_x) % groups_x
        py = (gy + off) % groups_y
        return px, py

    def for_peers(fn):
        def step(i, carry):
            fn(*peer(i))
            return carry

        lax.fori_loop(0, devices - groups_x, step, 0)
        lax.fori_loop(devices - groups_x + 1, devices, step, 0)

    barrier = pltpu.get_barrier_semaphore()
    for_peers(lambda px, py: pl.semaphore_signal(barrier, inc=1, device_id=(px, py), device_id_type=MESH))
    pl.semaphore_wait(barrier, devices - 1)

    def old_piece(chunk, part):
        state, sub = chunk // per_state, chunk % per_state
        row = pl.multiple_of((part // splits) * SUBLANES, SUBLANES)
        col = pl.multiple_of((part % splits) * span + sub * width, LANES)
        return olds[state].at[:, pl.ds(row, SUBLANES), pl.ds(col, width)]

    def own_rows(chunk):
        return by_rows[chunk].at[pl.ds(gx * held, held)]

    def first_copy(chunk, off):
        part = (gx + off) % groups_x
        return pltpu.make_async_remote_copy(
            src_ref=old_piece(chunk, part),
            dst_ref=own_rows(chunk),
            send_sem=send1.at[chunk, off],
            recv_sem=recv1.at[chunk, off],
            device_id=(part, gy),
            device_id_type=MESH,
        )

    def local_copy(chunk):
        return pltpu.make_async_copy(old_piece(chunk, gx), own_rows(chunk), local_sem.at[chunk])

    order = [sub + state * per_state for sub in range(per_state) for state in range(3)]
    for chunk in order:
        for off in range(1, groups_x):
            first_copy(chunk, off).start()
        local_copy(chunk).start()

    def count_copy(px, py):
        return pltpu.make_async_remote_copy(
            src_ref=count_row,
            dst_ref=all_counts.at[me],
            send_sem=send_c,
            recv_sem=recv_c,
            device_id=(px, py),
            device_id_type=MESH,
        )

    for_peers(lambda px, py: count_copy(px, py).start())
    all_counts[me] = count_row[...]

    def find(slot, carry):
        total = jnp.int32(0)
        for e in range(experts):
            total = total + jnp.where(new_owner[e] == slot, old_owner[e], 0)
        source[slot] = total
        return carry

    lax.fori_loop(0, experts, find, 0)

    def place(chunk):
        state, sub = chunk // per_state, chunk % per_state
        row = pl.multiple_of(gy * rows + (gx // splits) * SUBLANES, SUBLANES)
        col = pl.multiple_of((gx % splits) * span + sub * width, LANES)
        return state, row, col

    for chunk in order:
        local_copy(chunk).wait()
        for off in range(1, groups_x):
            first_copy(chunk, off).wait_recv()

        def stage(slot, carry):
            staged[chunk][slot] = by_rows[chunk][source[slot]]
            return carry

        lax.fori_loop(0, experts, stage, 0, unroll=4)
        state, row, col = place(chunk)

        def send(px, py):
            pltpu.make_async_remote_copy(
                src_ref=staged[chunk].at[px * groups_y + py],
                dst_ref=outs[state].at[0, pl.ds(row, SUBLANES), pl.ds(col, width)],
                send_sem=send2.at[chunk],
                recv_sem=recv2.at[chunk],
                device_id=(px, py),
                device_id_type=MESH,
            ).start()

        for_peers(send)
        outs[state][0, pl.ds(row, SUBLANES), pl.ds(col, width)] = by_rows[chunk][source[me]]

    others = all_counts.at[pl.ds(0, devices - 1)]
    pltpu.make_async_copy(others, others, recv_c).wait()
    totals = jnp.sum(all_counts[...], axis=0)
    count = jnp.sum(jnp.where(owner_row[...] == me, totals, 0.0), axis=1, keepdims=True)
    count_out[...] = jnp.broadcast_to(count, count_out.shape)

    for chunk in order:
        for off in range(1, groups_x):
            first_copy(chunk, off).wait_send()
    pltpu.make_async_copy(others, others, send_c).wait()
    for chunk in order:
        sent = staged[chunk].at[pl.ds(0, devices - 1)]
        pltpu.make_async_copy(sent, sent, send2.at[chunk]).wait()
        pltpu.make_async_copy(sent, sent, recv2.at[chunk]).wait()


def tiled_plan(groups_x, groups_y, shape, experts):
    held, rows, cols = shape
    if rows % SUBLANES or experts != groups_x * groups_y:
        return None
    tiles = rows // SUBLANES
    if groups_x % tiles:
        return None
    span = cols // (groups_x // tiles)
    if span % (LANES * SUBCHUNKS) or cols % span:
        return None
    return (groups_x, groups_y, experts, held, rows, tiles, span // SUBCHUNKS, 3 * SUBCHUNKS)


def kernel_body(dims, old_master, old_first, old_second, new_grad, counts, old_owner, new_owner):
    groups_x, groups_y, experts, held, rows, tiles, width, chunks = dims
    devices = groups_x * groups_y
    lanes = -(-experts // LANES) * LANES
    count_row = jnp.pad(counts.reshape(1, experts).astype(jnp.float32), ((0, 0), (0, lanes - experts)))
    owner_row = jnp.pad(new_owner.reshape(1, experts), ((0, 0), (0, lanes - experts)), constant_values=-1)
    tile = (1, rows * groups_y, old_master.shape[2])
    vmem = pl.BlockSpec(memory_space=pltpu.VMEM)
    smem = pl.BlockSpec(memory_space=pltpu.SMEM)
    hbm = pl.BlockSpec(memory_space=pl.ANY)
    buffers = [pltpu.VMEM((experts, SUBLANES, width), jnp.float32)] * (2 * chunks)
    master, first, second, count = pl.pallas_call(
        functools.partial(rehome_kernel, dims),
        out_shape=[jax.ShapeDtypeStruct(tile, jnp.float32)] * 3 + [jax.ShapeDtypeStruct((1, LANES), jnp.float32)],
        in_specs=[smem, smem, vmem, vmem, hbm, hbm, hbm],
        out_specs=[vmem] * 4,
        scratch_shapes=buffers
        + [
            pltpu.SMEM((experts,), jnp.int32),
            pltpu.VMEM((devices, 1, lanes), jnp.float32),
            pltpu.SemaphoreType.DMA((chunks,)),
            pltpu.SemaphoreType.DMA((chunks, groups_x)),
            pltpu.SemaphoreType.DMA((chunks, groups_x)),
            pltpu.SemaphoreType.DMA((chunks,)),
            pltpu.SemaphoreType.DMA((chunks,)),
            pltpu.SemaphoreType.DMA,
            pltpu.SemaphoreType.DMA,
        ],
        compiler_params=pltpu.CompilerParams(collective_id=0, has_side_effects=True),
    )(old_owner, new_owner, owner_row, count_row, old_master, old_first, old_second)
    return adam_step(master, first, second, new_grad, count[0, 0])


def body(old_master, old_first, old_second, new_grad, counts, old_owner, new_owner):
    dims = tiled_plan(lax.axis_size("gx"), lax.axis_size("gy"), old_master.shape, old_owner.shape[0])
    if dims is None:
        return plain_body(old_master, old_first, old_second, new_grad, counts, old_owner, new_owner)
    return kernel_body(dims, old_master, old_first, old_second, new_grad, counts, old_owner, new_owner)


def solution(mesh):
    placed = (
        P("gx", "gy", None),
        P("gx", "gy", None),
        P("gx", "gy", None),
        P(("gx", "gy"), None, None),
        P(None, ("gx", "gy")),
        P(),
        P(),
    )
    return jax.shard_map(
        body,
        mesh=mesh,
        in_specs=placed,
        out_specs=(P(("gx", "gy"), None, None),) * 3,
        check_vma=False,
    )
```

```python
import functools

import jax
import jax.numpy as jnp
from jax import lax
from jax.experimental import pallas as pl
from jax.experimental.pallas import tpu as pltpu
from jax.sharding import PartitionSpec as P

first_correction = 1.0 - 0.9**10
second_correction = 1.0 - 0.999**10
MESH = pl.DeviceIdType.MESH
LANES = 128
VMEM_GRANT = 8 << 20
SUBLANES = 8


def adam_step(master, first, second, grad, slot_count):
    scaled = grad.astype(jnp.float32) / slot_count
    new_first = 0.9 * first + 0.1 * scaled
    new_second = 0.999 * second + 0.001 * scaled * scaled
    step_dir = new_first / first_correction / (jnp.sqrt(new_second / second_correction) + 1e-08)
    new_master = master - 0.01 * (step_dir + 0.1 * master)
    return (new_master, new_first, new_second)


def reorder(block, groups_x, groups_y):
    total_rows = block.shape[1]
    piece = total_rows // (groups_x * groups_y)
    shaped = block.reshape(1, groups_x, groups_y, piece, block.shape[2])
    return shaped.transpose(0, 2, 1, 3, 4).reshape(1, total_rows, block.shape[2])


def plain_body(old_master, old_first, old_second, new_grad, counts, old_owner, new_owner):
    experts = old_owner.shape[0]
    groups_x = lax.axis_size("gx")
    groups_y = lax.axis_size("gy")
    my_slot = lax.axis_index("gx") * groups_y + lax.axis_index("gy")
    slots = jnp.arange(experts, dtype=jnp.int32)
    onehot = new_owner[:, None] == slots[None, :]
    source = jnp.sum(jnp.where(onehot, old_owner[:, None], 0), axis=0)
    local_counts = counts[:, 0].astype(jnp.float32)
    by_rows = tuple(
        lax.all_to_all(state, "gx", split_axis=1, concat_axis=0, tiled=True)
        for state in (old_master, old_first, old_second)
    )
    permuted = tuple((jnp.take(state, source, axis=0) for state in by_rows))
    landed = lax.all_to_all(permuted, ("gx", "gy"), split_axis=0, concat_axis=1, tiled=True)
    arrived = tuple((reorder(state, groups_x, groups_y) for state in landed))
    totals = lax.psum(local_counts, ("gx", "gy"))
    slot_count = jnp.sum(jnp.where(new_owner == my_slot, totals, jnp.float32(0.0)))
    return adam_step(arrived[0], arrived[1], arrived[2], new_grad, slot_count)


def rehome_kernel(dims, old_owner_hbm, new_owner_hbm, owner_row_hbm, count_row, old_m, old_f, old_s, *rest):
    groups_x, groups_y, experts, held, rows, tiles, span, pieces = dims
    chunks = len(pieces)
    outs, count_out = rest[:3], rest[3]
    by_rows = rest[4 : 4 + chunks]
    staged = rest[4 + chunks : 4 + 2 * chunks]
    (
        source, old_owner, new_owner, owner_row, all_counts, small_sem, local_sem, self_sem,
        send1, recv1, send2, recv2, send_c, recv_c,
    ) = rest[4 + 2 * chunks :]
    olds = (old_m, old_f, old_s)
    devices = groups_x * groups_y
    splits = groups_x // tiles
    gx = lax.axis_index("gx")
    gy = lax.axis_index("gy")
    me = gx * groups_y + gy

    def peer(i):
        at = i // groups_x
        sign = 1 - 2 * (at % 2)
        off = groups_y // 2 + sign * ((at + 1) // 2)
        px = (gx + i % groups_x) % groups_x
        py = (gy + off) % groups_y
        return px, py

    def for_peers(fn):
        def step(i, carry):
            fn(*peer(i))
            return carry

        lax.fori_loop(0, devices - groups_x, step, 0)
        lax.fori_loop(devices - groups_x + 1, devices, step, 0)

    small = (
        pltpu.make_async_copy(old_owner_hbm, old_owner, small_sem.at[0]),
        pltpu.make_async_copy(new_owner_hbm, new_owner, small_sem.at[1]),
        pltpu.make_async_copy(owner_row_hbm, owner_row, small_sem.at[2]),
        pltpu.make_async_copy(count_row, all_counts.at[me], small_sem.at[3]),
    )
    for copy in small:
        copy.start()

    barrier = pltpu.get_barrier_semaphore()
    for_peers(lambda px, py: pl.semaphore_signal(barrier, inc=1, device_id=(px, py), device_id_type=MESH))
    pl.semaphore_wait(barrier, devices - 1)

    def old_piece(chunk, part):
        state, start, width = pieces[chunk]
        row = pl.multiple_of((part // splits) * SUBLANES, SUBLANES)
        col = pl.multiple_of((part % splits) * span + start, LANES)
        return olds[state].at[:, pl.ds(row, SUBLANES), pl.ds(col, width)]

    def own_rows(chunk):
        return by_rows[chunk].at[pl.ds(gx * held, held)]

    def first_copy(chunk, off):
        part = (gx + off) % groups_x
        return pltpu.make_async_remote_copy(
            src_ref=old_piece(chunk, part),
            dst_ref=own_rows(chunk),
            send_sem=send1.at[chunk, off],
            recv_sem=recv1.at[chunk, off],
            device_id=(part, gy),
            device_id_type=MESH,
        )

    def local_copy(chunk):
        return pltpu.make_async_copy(old_piece(chunk, gx), own_rows(chunk), local_sem.at[chunk])

    order = range(chunks)
    for chunk in order:
        for off in range(1, groups_x):
            first_copy(chunk, off).start()
        local_copy(chunk).start()

    def count_copy(px, py):
        return pltpu.make_async_remote_copy(
            src_ref=count_row,
            dst_ref=all_counts.at[me],
            send_sem=send_c,
            recv_sem=recv_c,
            device_id=(px, py),
            device_id_type=MESH,
        )

    for_peers(lambda px, py: count_copy(px, py).start())
    for copy in small:
        copy.wait()

    def find(slot, carry):
        total = jnp.int32(0)
        for e in range(experts):
            total = total + jnp.where(new_owner[e] == slot, old_owner[e], 0)
        source[slot] = total
        return carry

    lax.fori_loop(0, experts, find, 0)

    def landing(chunk):
        state, start, width = pieces[chunk]
        row = pl.multiple_of(gy * rows + (gx // splits) * SUBLANES, SUBLANES)
        col = pl.multiple_of((gx % splits) * span + start, LANES)
        return outs[state].at[0, pl.ds(row, SUBLANES), pl.ds(col, width)]

    def self_copy(chunk):
        return pltpu.make_async_copy(staged[chunk].at[me], landing(chunk), self_sem.at[chunk])

    for chunk in order:
        local_copy(chunk).wait()
        for off in range(1, groups_x):
            first_copy(chunk, off).wait_recv()

        def stage(slot, carry):
            staged[chunk][slot] = by_rows[chunk][source[slot]]
            return carry

        lax.fori_loop(0, experts, stage, 0, unroll=4)

        def send(px, py):
            pltpu.make_async_remote_copy(
                src_ref=staged[chunk].at[px * groups_y + py],
                dst_ref=landing(chunk),
                send_sem=send2.at[chunk],
                recv_sem=recv2.at[chunk],
                device_id=(px, py),
                device_id_type=MESH,
            ).start()

        for_peers(send)
        self_copy(chunk).start()

    others = all_counts.at[pl.ds(0, devices - 1)]
    pltpu.make_async_copy(others, others, recv_c).wait()
    totals = jnp.sum(all_counts[...].astype(jnp.float32), axis=0)
    count = jnp.sum(jnp.where(owner_row[...] == me, totals, 0.0), axis=1, keepdims=True)
    count_out[...] = jnp.broadcast_to(count, count_out.shape)

    for chunk in order:
        for off in range(1, groups_x):
            first_copy(chunk, off).wait_send()
    pltpu.make_async_copy(others, others, send_c).wait()
    for chunk in order:
        self_copy(chunk).wait()
        sent = staged[chunk].at[pl.ds(0, devices - 1)]
        pltpu.make_async_copy(sent, sent, send2.at[chunk]).wait()
        pltpu.make_async_copy(sent, sent, recv2.at[chunk]).wait()


def tiled_plan(groups_x, groups_y, shape, experts):
    held, rows, cols = shape
    if rows % SUBLANES or experts != groups_x * groups_y:
        return None
    tiles = rows // SUBLANES
    if groups_x % tiles:
        return None
    span = cols // (groups_x // tiles)
    if span % LANES:
        return None
    half = (span // LANES + 1) // 2 * LANES
    pieces = [(state, 0, half) for state in range(3)]
    if half < span:
        pieces += [(state, half, span - half) for state in range(3)]
    if half > LANES:
        pieces[:1] = [(0, 0, LANES), (0, LANES, half - LANES)]
    return (groups_x, groups_y, experts, held, rows, tiles, span, tuple(pieces))


def kernel_body(dims, old_master, old_first, old_second, new_grad, counts, old_owner, new_owner):
    groups_x, groups_y, experts, held, rows, tiles, span, pieces = dims
    devices = groups_x * groups_y
    chunks = len(pieces)
    tile = (1, rows * groups_y, old_master.shape[2])
    vmem = pl.BlockSpec(memory_space=pltpu.VMEM)
    anywhere = pl.BlockSpec(memory_space=pl.ANY)
    buffers = [pltpu.VMEM((experts, SUBLANES, width), jnp.float32) for _, _, width in pieces] * 2
    master, first, second, count = pl.pallas_call(
        functools.partial(rehome_kernel, dims),
        out_shape=[jax.ShapeDtypeStruct(tile, jnp.float32)] * 3 + [jax.ShapeDtypeStruct((1, LANES), jnp.float32)],
        in_specs=[pl.BlockSpec(memory_space=pltpu.HBM)] * 7,
        out_specs=[anywhere] * 3 + [vmem],
        scratch_shapes=buffers
        + [
            pltpu.SMEM((experts,), jnp.int32),
            pltpu.SMEM((experts,), jnp.int32),
            pltpu.SMEM((experts,), jnp.int32),
            pltpu.VMEM((1, experts), jnp.int32),
            pltpu.VMEM((devices, 1, experts), jnp.int32),
            pltpu.SemaphoreType.DMA((4,)),
            pltpu.SemaphoreType.DMA((chunks,)),
            pltpu.SemaphoreType.DMA((chunks,)),
            pltpu.SemaphoreType.DMA((chunks, groups_x)),
            pltpu.SemaphoreType.DMA((chunks, groups_x)),
            pltpu.SemaphoreType.DMA((chunks,)),
            pltpu.SemaphoreType.DMA((chunks,)),
            pltpu.SemaphoreType.DMA,
            pltpu.SemaphoreType.DMA,
        ],
        compiler_params=pltpu.CompilerParams(collective_id=0, has_side_effects=True, vmem_limit_bytes=VMEM_GRANT),
    )(
        old_owner,
        new_owner,
        new_owner.reshape(1, experts),
        counts.reshape(1, experts),
        old_master,
        old_first,
        old_second,
    )
    return adam_step(master, first, second, new_grad, count[0, 0])


def body(old_master, old_first, old_second, new_grad, counts, old_owner, new_owner):
    dims = tiled_plan(lax.axis_size("gx"), lax.axis_size("gy"), old_master.shape, old_owner.shape[0])
    if dims is None:
        return plain_body(old_master, old_first, old_second, new_grad, counts, old_owner, new_owner)
    return kernel_body(dims, old_master, old_first, old_second, new_grad, counts, old_owner, new_owner)


def solution(mesh):
    placed = (
        P("gx", "gy", None),
        P("gx", "gy", None),
        P("gx", "gy", None),
        P(("gx", "gy"), None, None),
        P(None, ("gx", "gy")),
        P(),
        P(),
    )
    return jax.shard_map(
        body,
        mesh=mesh,
        in_specs=placed,
        out_specs=(P(("gx", "gy"), None, None),) * 3,
        check_vma=False,
    )
```

```python
import functools

import jax
import jax.numpy as jnp
from jax import lax
from jax.experimental import pallas as pl
from jax.experimental.pallas import tpu as pltpu
from jax.sharding import PartitionSpec as P

first_correction = 1.0 - 0.9**10
second_correction = 1.0 - 0.999**10
MESH = pl.DeviceIdType.MESH
LANES = 128
VMEM_GRANT = 10 << 20
SUBLANES = 8


def adam_step(master, first, second, grad, slot_count):
    scaled = grad.astype(jnp.float32) / slot_count
    new_first = 0.9 * first + 0.1 * scaled
    new_second = 0.999 * second + 0.001 * scaled * scaled
    step_dir = new_first / first_correction / (jnp.sqrt(new_second / second_correction) + 1e-08)
    new_master = master - 0.01 * (step_dir + 0.1 * master)
    return (new_master, new_first, new_second)


def reorder(block, groups_x, groups_y):
    total_rows = block.shape[1]
    piece = total_rows // (groups_x * groups_y)
    shaped = block.reshape(1, groups_x, groups_y, piece, block.shape[2])
    return shaped.transpose(0, 2, 1, 3, 4).reshape(1, total_rows, block.shape[2])


def plain_body(old_master, old_first, old_second, new_grad, counts, old_owner, new_owner):
    experts = old_owner.shape[0]
    groups_x = lax.axis_size("gx")
    groups_y = lax.axis_size("gy")
    my_slot = lax.axis_index("gx") * groups_y + lax.axis_index("gy")
    slots = jnp.arange(experts, dtype=jnp.int32)
    onehot = new_owner[:, None] == slots[None, :]
    source = jnp.sum(jnp.where(onehot, old_owner[:, None], 0), axis=0)
    local_counts = counts[:, 0].astype(jnp.float32)
    by_rows = tuple(
        lax.all_to_all(state, "gx", split_axis=1, concat_axis=0, tiled=True)
        for state in (old_master, old_first, old_second)
    )
    permuted = tuple((jnp.take(state, source, axis=0) for state in by_rows))
    landed = lax.all_to_all(permuted, ("gx", "gy"), split_axis=0, concat_axis=1, tiled=True)
    arrived = tuple((reorder(state, groups_x, groups_y) for state in landed))
    totals = lax.psum(local_counts, ("gx", "gy"))
    slot_count = jnp.sum(jnp.where(new_owner == my_slot, totals, jnp.float32(0.0)))
    return adam_step(arrived[0], arrived[1], arrived[2], new_grad, slot_count)


def rehome_kernel(dims, old_owner_hbm, new_owner_hbm, owner_row_hbm, count_row, old_m, old_f, old_s, *rest):
    groups_x, groups_y, experts, held, rows, tiles, span, pieces = dims
    chunks = len(pieces)
    outs, count_out = rest[:3], rest[3]
    by_rows = rest[4 : 4 + chunks]
    staged = rest[4 + chunks : 4 + 2 * chunks]
    ready = rest[4 + 2 * chunks : 4 + 3 * chunks]
    (
        source, old_owner, new_owner, owner_row, all_counts, small_sem, local_sem, self_sem,
        send1, recv1, send2, recv2, send_c, recv_c,
    ) = rest[4 + 3 * chunks :]
    olds = (old_m, old_f, old_s)
    devices = groups_x * groups_y
    splits = groups_x // tiles
    gx = lax.axis_index("gx")
    gy = lax.axis_index("gy")
    me = gx * groups_y + gy

    peers_x = [(gx + off) % groups_x for off in range(groups_x)]
    offsets = sorted(range(groups_y), key=lambda off: (-min(off, groups_y - off), off))
    peers_y = {off: (gy + off) % groups_y for off in offsets}

    def for_peers(fn):
        for off_y in offsets:
            for off_x in range(groups_x):
                if off_x or off_y:
                    fn(peers_x[off_x], peers_y[off_y])

    small = (
        pltpu.make_async_copy(old_owner_hbm, old_owner, small_sem.at[0]),
        pltpu.make_async_copy(new_owner_hbm, new_owner, small_sem.at[1]),
        pltpu.make_async_copy(owner_row_hbm, owner_row, small_sem.at[2]),
        pltpu.make_async_copy(count_row, all_counts.at[me], small_sem.at[3]),
    )
    barrier = pltpu.get_barrier_semaphore()
    for_peers(lambda px, py: pl.semaphore_signal(barrier, inc=1, device_id=(px, py), device_id_type=MESH))

    for copy in small:
        copy.start()

    def old_piece(chunk, part):
        state, start, width = pieces[chunk]
        row = pl.multiple_of((part // splits) * SUBLANES, SUBLANES)
        col = pl.multiple_of((part % splits) * span + start, LANES)
        return olds[state].at[:, pl.ds(row, SUBLANES), pl.ds(col, width)]

    def own_rows(chunk):
        return by_rows[chunk].at[pl.ds(gx * held, held)]

    def local_copy(chunk, off):
        target = own_rows(chunk) if off == 0 else ready[chunk].at[off - 1]
        return pltpu.make_async_copy(old_piece(chunk, peers_x[off]), target, local_sem.at[chunk, off])

    def first_copy(chunk, off):
        return pltpu.make_async_remote_copy(
            src_ref=ready[chunk].at[off - 1],
            dst_ref=own_rows(chunk),
            send_sem=send1.at[chunk, off],
            recv_sem=recv1.at[chunk, off],
            device_id=(peers_x[off], gy),
            device_id_type=MESH,
        )

    order = range(chunks)
    for chunk in order:
        for off in [*range(1, groups_x), 0]:
            local_copy(chunk, off).start()

    for copy in small:
        copy.wait()

    owners = [new_owner[e] for e in range(experts)]
    places = [old_owner[e] for e in range(experts)]

    def find(slot, carry):
        total = jnp.int32(0)
        for e in range(experts):
            total = total + jnp.where(owners[e] == slot, places[e], 0)
        source[slot] = total
        return carry

    lax.fori_loop(0, experts, find, 0)

    pl.semaphore_wait(barrier, devices - 1)

    for chunk in order:
        for off in range(1, groups_x):
            local_copy(chunk, off).wait()
            first_copy(chunk, off).start()

    def count_copy(px, py):
        return pltpu.make_async_remote_copy(
            src_ref=count_row,
            dst_ref=all_counts.at[me],
            send_sem=send_c,
            recv_sem=recv_c,
            device_id=(px, py),
            device_id_type=MESH,
        )

    for_peers(lambda px, py: count_copy(px, py).start())
    def landing(chunk):
        state, start, width = pieces[chunk]
        row = pl.multiple_of(gy * rows + (gx // splits) * SUBLANES, SUBLANES)
        col = pl.multiple_of((gx % splits) * span + start, LANES)
        return outs[state].at[0, pl.ds(row, SUBLANES), pl.ds(col, width)]

    def self_copy(chunk):
        return pltpu.make_async_copy(staged[chunk].at[me], landing(chunk), self_sem.at[chunk])

    for chunk in order:
        local_copy(chunk, 0).wait()
        for off in range(1, groups_x):
            first_copy(chunk, off).wait_recv()

        def stage(slot, carry):
            staged[chunk][slot] = by_rows[chunk][source[slot]]
            return carry

        lax.fori_loop(0, experts, stage, 0, unroll=4)

        def send(px, py):
            pltpu.make_async_remote_copy(
                src_ref=staged[chunk].at[px * groups_y + py],
                dst_ref=landing(chunk),
                send_sem=send2.at[chunk],
                recv_sem=recv2.at[chunk],
                device_id=(px, py),
                device_id_type=MESH,
            ).start()

        for_peers(send)
        self_copy(chunk).start()

    others = all_counts.at[pl.ds(0, devices - 1)]
    pltpu.make_async_copy(others, others, recv_c).wait()
    totals = jnp.sum(all_counts[...].astype(jnp.float32), axis=0)
    count = jnp.sum(jnp.where(owner_row[...] == me, totals, 0.0), axis=1, keepdims=True)
    count_out[...] = jnp.broadcast_to(count, count_out.shape)

    for chunk in order:
        for off in range(1, groups_x):
            first_copy(chunk, off).wait_send()
    pltpu.make_async_copy(others, others, send_c).wait()
    for chunk in order:
        self_copy(chunk).wait()
        sent = staged[chunk].at[pl.ds(0, devices - 1)]
        pltpu.make_async_copy(sent, sent, send2.at[chunk]).wait()
        pltpu.make_async_copy(sent, sent, recv2.at[chunk]).wait()


def tiled_plan(groups_x, groups_y, shape, experts):
    held, rows, cols = shape
    if rows % SUBLANES or experts != groups_x * groups_y:
        return None
    tiles = rows // SUBLANES
    if groups_x % tiles:
        return None
    span = cols // (groups_x // tiles)
    if span % LANES:
        return None
    half = (span // LANES + 1) // 2 * LANES
    pieces = [(state, 0, half) for state in range(3)]
    if half < span:
        pieces += [(state, half, span - half) for state in range(3)]
    if half > LANES:
        pieces[:1] = [(0, 0, LANES), (0, LANES, half - LANES)]
    return (groups_x, groups_y, experts, held, rows, tiles, span, tuple(pieces))


def kernel_body(dims, old_master, old_first, old_second, new_grad, counts, old_owner, new_owner):
    groups_x, groups_y, experts, held, rows, tiles, span, pieces = dims
    devices = groups_x * groups_y
    chunks = len(pieces)
    tile = (1, rows * groups_y, old_master.shape[2])
    vmem = pl.BlockSpec(memory_space=pltpu.VMEM)
    anywhere = pl.BlockSpec(memory_space=pl.ANY)
    buffers = [pltpu.VMEM((experts, SUBLANES, width), jnp.float32) for _, _, width in pieces] * 2
    buffers += [pltpu.VMEM((groups_x - 1, held, SUBLANES, width), jnp.float32) for _, _, width in pieces]
    row = new_owner.reshape(1, experts)
    operands = (old_owner, new_owner, row, counts.reshape(1, experts), old_master, old_first, old_second)
    kept = [pltpu.with_memory_space_constraint(array, pltpu.HBM) for array in operands]
    master, first, second, count = pl.pallas_call(
        functools.partial(rehome_kernel, dims),
        out_shape=[jax.ShapeDtypeStruct(tile, jnp.float32)] * 3 + [jax.ShapeDtypeStruct((1, LANES), jnp.float32)],
        in_specs=[pl.BlockSpec(memory_space=pltpu.HBM)] * 7,
        out_specs=[anywhere] * 3 + [vmem],
        scratch_shapes=buffers
        + [
            pltpu.SMEM((experts,), jnp.int32),
            pltpu.SMEM((experts,), jnp.int32),
            pltpu.SMEM((experts,), jnp.int32),
            pltpu.VMEM((1, experts), jnp.int32),
            pltpu.VMEM((devices, 1, experts), jnp.int32),
            pltpu.SemaphoreType.DMA((4,)),
            pltpu.SemaphoreType.DMA((chunks, groups_x)),
            pltpu.SemaphoreType.DMA((chunks,)),
            pltpu.SemaphoreType.DMA((chunks, groups_x)),
            pltpu.SemaphoreType.DMA((chunks, groups_x)),
            pltpu.SemaphoreType.DMA((chunks,)),
            pltpu.SemaphoreType.DMA((chunks,)),
            pltpu.SemaphoreType.DMA,
            pltpu.SemaphoreType.DMA,
        ],
        compiler_params=pltpu.CompilerParams(collective_id=0, has_side_effects=True, vmem_limit_bytes=VMEM_GRANT),
    )(*kept)
    return adam_step(master, first, second, new_grad, count[0, 0])


def body(old_master, old_first, old_second, new_grad, counts, old_owner, new_owner):
    dims = tiled_plan(lax.axis_size("gx"), lax.axis_size("gy"), old_master.shape, old_owner.shape[0])
    if dims is None:
        return plain_body(old_master, old_first, old_second, new_grad, counts, old_owner, new_owner)
    return kernel_body(dims, old_master, old_first, old_second, new_grad, counts, old_owner, new_owner)


def solution(mesh):
    placed = (
        P("gx", "gy", None),
        P("gx", "gy", None),
        P("gx", "gy", None),
        P(("gx", "gy"), None, None),
        P(None, ("gx", "gy")),
        P(),
        P(),
    )
    return jax.shard_map(
        body,
        mesh=mesh,
        in_specs=placed,
        out_specs=(P(("gx", "gy"), None, None),) * 3,
        check_vma=False,
    )
```

```python
import functools

import jax
import jax.numpy as jnp
from jax import lax
from jax.experimental import pallas as pl
from jax.experimental.pallas import tpu as pltpu
from jax.sharding import PartitionSpec as P

first_correction = 1.0 - 0.9**10
second_correction = 1.0 - 0.999**10
MESH = pl.DeviceIdType.MESH
LANES = 128
VMEM_GRANT = 10 << 20
SUBLANES = 8


def adam_step(master, first, second, grad, slot_count):
    scaled = grad.astype(jnp.float32) / slot_count
    new_first = 0.9 * first + 0.1 * scaled
    new_second = 0.999 * second + 0.001 * scaled * scaled
    step_dir = new_first / first_correction / (jnp.sqrt(new_second / second_correction) + 1e-08)
    new_master = master - 0.01 * (step_dir + 0.1 * master)
    return (new_master, new_first, new_second)


def reorder(block, groups_x, groups_y):
    total_rows = block.shape[1]
    piece = total_rows // (groups_x * groups_y)
    shaped = block.reshape(1, groups_x, groups_y, piece, block.shape[2])
    return shaped.transpose(0, 2, 1, 3, 4).reshape(1, total_rows, block.shape[2])


def plain_body(old_master, old_first, old_second, new_grad, counts, old_owner, new_owner):
    experts = old_owner.shape[0]
    groups_x = lax.axis_size("gx")
    groups_y = lax.axis_size("gy")
    my_slot = lax.axis_index("gx") * groups_y + lax.axis_index("gy")
    slots = jnp.arange(experts, dtype=jnp.int32)
    onehot = new_owner[:, None] == slots[None, :]
    source = jnp.sum(jnp.where(onehot, old_owner[:, None], 0), axis=0)
    local_counts = counts[:, 0].astype(jnp.float32)
    by_rows = tuple(
        lax.all_to_all(state, "gx", split_axis=1, concat_axis=0, tiled=True)
        for state in (old_master, old_first, old_second)
    )
    permuted = tuple((jnp.take(state, source, axis=0) for state in by_rows))
    landed = lax.all_to_all(permuted, ("gx", "gy"), split_axis=0, concat_axis=1, tiled=True)
    arrived = tuple((reorder(state, groups_x, groups_y) for state in landed))
    totals = lax.psum(local_counts, ("gx", "gy"))
    slot_count = jnp.sum(jnp.where(new_owner == my_slot, totals, jnp.float32(0.0)))
    return adam_step(arrived[0], arrived[1], arrived[2], new_grad, slot_count)


def rehome_kernel(dims, old_owner_hbm, new_owner_hbm, owner_row_hbm, count_row, old_m, old_f, old_s, *rest):
    groups_x, groups_y, experts, held, rows, tiles, span, pieces = dims
    chunks = len(pieces)
    outs, count_out = rest[:3], rest[3]
    by_rows = rest[4 : 4 + chunks]
    staged = rest[4 + chunks : 4 + 2 * chunks]
    ready = rest[4 + 2 * chunks : 4 + 3 * chunks]
    (
        source, old_owner, new_owner, owner_row, all_counts, small_sem, local_sem, self_sem,
        send1, recv1, send2, recv2, send_c, recv_c, row_in,
    ) = rest[4 + 3 * chunks :]
    olds = (old_m, old_f, old_s)
    devices = groups_x * groups_y
    splits = groups_x // tiles
    gx = lax.axis_index("gx")
    gy = lax.axis_index("gy")
    me = gx * groups_y + gy

    peers_x = [(gx + off) % groups_x for off in range(groups_x)]
    offsets = sorted(range(groups_y), key=lambda off: (-min(off, groups_y - off), off))
    peers_y = {off: (gy + off) % groups_y for off in offsets}

    def for_peers(fn):
        for off_y in offsets:
            for off_x in range(groups_x):
                if off_x or off_y:
                    fn(peers_x[off_x], peers_y[off_y])

    small = (
        pltpu.make_async_copy(old_owner_hbm, old_owner, small_sem.at[0]),
        pltpu.make_async_copy(new_owner_hbm, new_owner, small_sem.at[1]),
        pltpu.make_async_copy(owner_row_hbm, owner_row, small_sem.at[2]),
        pltpu.make_async_copy(count_row, all_counts.at[me], small_sem.at[3]),
    )
    barrier = pltpu.get_barrier_semaphore()
    for off_y in offsets[:-1]:
        pl.semaphore_signal(barrier, inc=1, device_id=(gx, peers_y[off_y]), device_id_type=MESH)
    for off_x in range(1, groups_x):
        pl.semaphore_signal(barrier, inc=1, device_id=(peers_x[off_x], gy), device_id_type=MESH)

    for copy in small:
        copy.start()

    def old_piece(chunk, part):
        state, start, width = pieces[chunk]
        row = pl.multiple_of((part // splits) * SUBLANES, SUBLANES)
        col = pl.multiple_of((part % splits) * span + start, LANES)
        return olds[state].at[:, pl.ds(row, SUBLANES), pl.ds(col, width)]

    def own_rows(chunk):
        return by_rows[chunk].at[pl.ds(gx * held, held)]

    def local_copy(chunk, off):
        target = own_rows(chunk) if off == 0 else ready[chunk].at[off - 1]
        return pltpu.make_async_copy(old_piece(chunk, peers_x[off]), target, local_sem.at[chunk, off])

    def first_copy(chunk, off):
        return pltpu.make_async_remote_copy(
            src_ref=ready[chunk].at[off - 1],
            dst_ref=own_rows(chunk),
            send_sem=send1.at[chunk, off],
            recv_sem=recv1.at[chunk, off],
            device_id=(peers_x[off], gy),
            device_id_type=MESH,
        )

    order = range(chunks)
    for chunk in order:
        for off in [*range(1, groups_x), 0]:
            local_copy(chunk, off).start()

    pl.semaphore_wait(barrier, groups_x + groups_y - 2)
    for off_x in range(1, groups_x):
        pl.semaphore_signal(row_in, inc=1, device_id=(peers_x[off_x], gy), device_id_type=MESH)

    for chunk in order:
        for off in range(1, groups_x):
            local_copy(chunk, off).wait()
            first_copy(chunk, off).start()

    for copy in small:
        copy.wait()

    owners = [new_owner[e] for e in range(experts)]
    places = [old_owner[e] for e in range(experts)]

    def find(slot, carry):
        total = jnp.int32(0)
        for e in range(experts):
            total = total + jnp.where(owners[e] == slot, places[e], 0)
        source[slot] = total
        return carry

    lax.fori_loop(0, experts, find, 0)

    def count_copy(px, py):
        return pltpu.make_async_remote_copy(
            src_ref=count_row,
            dst_ref=all_counts.at[me],
            send_sem=send_c,
            recv_sem=recv_c,
            device_id=(px, py),
            device_id_type=MESH,
        )

    pl.semaphore_wait(row_in, groups_x - 1)
    def landing(chunk):
        state, start, width = pieces[chunk]
        row = pl.multiple_of(gy * rows + (gx // splits) * SUBLANES, SUBLANES)
        col = pl.multiple_of((gx % splits) * span + start, LANES)
        return outs[state].at[0, pl.ds(row, SUBLANES), pl.ds(col, width)]

    def self_copy(chunk):
        return pltpu.make_async_copy(staged[chunk].at[me], landing(chunk), self_sem.at[chunk])

    for chunk in order:
        local_copy(chunk, 0).wait()
        for off in range(1, groups_x):
            first_copy(chunk, off).wait_recv()

        def stage(slot, carry):
            staged[chunk][slot] = by_rows[chunk][source[slot]]
            return carry

        lax.fori_loop(0, experts, stage, 0, unroll=4)

        def send(px, py):
            pltpu.make_async_remote_copy(
                src_ref=staged[chunk].at[px * groups_y + py],
                dst_ref=landing(chunk),
                send_sem=send2.at[chunk],
                recv_sem=recv2.at[chunk],
                device_id=(px, py),
                device_id_type=MESH,
            ).start()

        for_peers(send)
        self_copy(chunk).start()
        if chunk == 0:
            for_peers(lambda px, py: count_copy(px, py).start())

    others = all_counts.at[pl.ds(0, devices - 1)]
    pltpu.make_async_copy(others, others, recv_c).wait()
    totals = jnp.sum(all_counts[...].astype(jnp.float32), axis=0)
    count = jnp.sum(jnp.where(owner_row[...] == me, totals, 0.0), axis=1, keepdims=True)
    count_out[...] = jnp.broadcast_to(count, count_out.shape)

    for chunk in order:
        for off in range(1, groups_x):
            first_copy(chunk, off).wait_send()
    pltpu.make_async_copy(others, others, send_c).wait()
    for chunk in order:
        self_copy(chunk).wait()
        sent = staged[chunk].at[pl.ds(0, devices - 1)]
        pltpu.make_async_copy(sent, sent, send2.at[chunk]).wait()
        pltpu.make_async_copy(sent, sent, recv2.at[chunk]).wait()


def tiled_plan(groups_x, groups_y, shape, experts):
    held, rows, cols = shape
    if rows % SUBLANES or experts != groups_x * groups_y:
        return None
    tiles = rows // SUBLANES
    if groups_x % tiles:
        return None
    span = cols // (groups_x // tiles)
    if span % LANES:
        return None
    half = (span // LANES + 1) // 2 * LANES
    pieces = [(state, 0, half) for state in range(3)]
    if half < span:
        pieces += [(state, half, span - half) for state in range(3)]
    if half > LANES:
        pieces[:1] = [(0, 0, LANES), (0, LANES, half - LANES)]
    return (groups_x, groups_y, experts, held, rows, tiles, span, tuple(pieces))


def kernel_body(dims, old_master, old_first, old_second, new_grad, counts, old_owner, new_owner):
    groups_x, groups_y, experts, held, rows, tiles, span, pieces = dims
    devices = groups_x * groups_y
    chunks = len(pieces)
    tile = (1, rows * groups_y, old_master.shape[2])
    vmem = pl.BlockSpec(memory_space=pltpu.VMEM)
    anywhere = pl.BlockSpec(memory_space=pl.ANY)
    buffers = [pltpu.VMEM((experts, SUBLANES, width), jnp.float32) for _, _, width in pieces] * 2
    buffers += [pltpu.VMEM((groups_x - 1, held, SUBLANES, width), jnp.float32) for _, _, width in pieces]
    row = new_owner.reshape(1, experts)
    operands = (old_owner, new_owner, row, counts.reshape(1, experts), old_master, old_first, old_second)
    kept = [pltpu.with_memory_space_constraint(array, pltpu.HBM) for array in operands]
    master, first, second, count = pl.pallas_call(
        functools.partial(rehome_kernel, dims),
        out_shape=[jax.ShapeDtypeStruct(tile, jnp.float32)] * 3 + [jax.ShapeDtypeStruct((1, LANES), jnp.float32)],
        in_specs=[pl.BlockSpec(memory_space=pltpu.HBM)] * 7,
        out_specs=[anywhere] * 3 + [vmem],
        scratch_shapes=buffers
        + [
            pltpu.SMEM((experts,), jnp.int32),
            pltpu.SMEM((experts,), jnp.int32),
            pltpu.SMEM((experts,), jnp.int32),
            pltpu.VMEM((1, experts), jnp.int32),
            pltpu.VMEM((devices, 1, experts), jnp.int32),
            pltpu.SemaphoreType.DMA((4,)),
            pltpu.SemaphoreType.DMA((chunks, groups_x)),
            pltpu.SemaphoreType.DMA((chunks,)),
            pltpu.SemaphoreType.DMA((chunks, groups_x)),
            pltpu.SemaphoreType.DMA((chunks, groups_x)),
            pltpu.SemaphoreType.DMA((chunks,)),
            pltpu.SemaphoreType.DMA((chunks,)),
            pltpu.SemaphoreType.DMA,
            pltpu.SemaphoreType.DMA,
            pltpu.SemaphoreType.REGULAR,
        ],
        compiler_params=pltpu.CompilerParams(collective_id=0, has_side_effects=True, vmem_limit_bytes=VMEM_GRANT),
    )(*kept)
    return adam_step(master, first, second, new_grad, count[0, 0])


def body(old_master, old_first, old_second, new_grad, counts, old_owner, new_owner):
    dims = tiled_plan(lax.axis_size("gx"), lax.axis_size("gy"), old_master.shape, old_owner.shape[0])
    if dims is None:
        return plain_body(old_master, old_first, old_second, new_grad, counts, old_owner, new_owner)
    return kernel_body(dims, old_master, old_first, old_second, new_grad, counts, old_owner, new_owner)


def solution(mesh):
    placed = (
        P("gx", "gy", None),
        P("gx", "gy", None),
        P("gx", "gy", None),
        P(("gx", "gy"), None, None),
        P(None, ("gx", "gy")),
        P(),
        P(),
    )
    return jax.shard_map(
        body,
        mesh=mesh,
        in_specs=placed,
        out_specs=(P(("gx", "gy"), None, None),) * 3,
        check_vma=False,
    )
```

```python
import functools

import jax
import jax.numpy as jnp
from jax import lax
from jax.experimental import pallas as pl
from jax.experimental.pallas import tpu as pltpu
from jax.sharding import PartitionSpec as P

first_correction = 1.0 - 0.9**10
second_correction = 1.0 - 0.999**10
MESH = pl.DeviceIdType.MESH
LANES = 128
VMEM_GRANT = 10 << 20
SUBLANES = 8


def adam_step(master, first, second, grad, slot_count):
    scaled = grad.astype(jnp.float32) / slot_count
    new_first = 0.9 * first + 0.1 * scaled
    new_second = 0.999 * second + 0.001 * scaled * scaled
    step_dir = new_first / first_correction / (jnp.sqrt(new_second / second_correction) + 1e-08)
    new_master = master - 0.01 * (step_dir + 0.1 * master)
    return (new_master, new_first, new_second)


def reorder(block, groups_x, groups_y):
    total_rows = block.shape[1]
    piece = total_rows // (groups_x * groups_y)
    shaped = block.reshape(1, groups_x, groups_y, piece, block.shape[2])
    return shaped.transpose(0, 2, 1, 3, 4).reshape(1, total_rows, block.shape[2])


def plain_body(old_master, old_first, old_second, new_grad, counts, old_owner, new_owner):
    experts = old_owner.shape[0]
    groups_x = lax.axis_size("gx")
    groups_y = lax.axis_size("gy")
    my_slot = lax.axis_index("gx") * groups_y + lax.axis_index("gy")
    slots = jnp.arange(experts, dtype=jnp.int32)
    onehot = new_owner[:, None] == slots[None, :]
    source = jnp.sum(jnp.where(onehot, old_owner[:, None], 0), axis=0)
    local_counts = counts[:, 0].astype(jnp.float32)
    by_rows = tuple(
        lax.all_to_all(state, "gx", split_axis=1, concat_axis=0, tiled=True)
        for state in (old_master, old_first, old_second)
    )
    permuted = tuple((jnp.take(state, source, axis=0) for state in by_rows))
    landed = lax.all_to_all(permuted, ("gx", "gy"), split_axis=0, concat_axis=1, tiled=True)
    arrived = tuple((reorder(state, groups_x, groups_y) for state in landed))
    totals = lax.psum(local_counts, ("gx", "gy"))
    slot_count = jnp.sum(jnp.where(new_owner == my_slot, totals, jnp.float32(0.0)))
    return adam_step(arrived[0], arrived[1], arrived[2], new_grad, slot_count)


def rehome_kernel(dims, old_owner_hbm, new_owner_hbm, owner_row_hbm, count_row, old_m, old_f, old_s, *rest):
    groups_x, groups_y, experts, held, rows, tiles, span, pieces = dims
    chunks = len(pieces)
    outs, count_out = rest[:3], rest[3]
    by_rows = rest[4 : 4 + chunks]
    staged = rest[4 + chunks : 4 + 2 * chunks]
    ready = rest[4 + 2 * chunks : 4 + 3 * chunks]
    (
        source, old_owner, new_owner, owner_row, all_counts, small_sem, local_sem, self_sem,
        send1, recv1, send2, recv2, send_c, recv_c, row_in,
    ) = rest[4 + 3 * chunks :]
    olds = (old_m, old_f, old_s)
    devices = groups_x * groups_y
    splits = groups_x // tiles
    gx = lax.axis_index("gx")
    gy = lax.axis_index("gy")
    me = gx * groups_y + gy

    peers_x = [(gx + off) % groups_x for off in range(groups_x)]
    offsets = sorted(range(groups_y), key=lambda off: (-min(off, groups_y - off), off))
    peers_y = {off: (gy + off) % groups_y for off in offsets}

    def for_peers(fn):
        for off_y in offsets:
            for off_x in range(groups_x):
                if off_x or off_y:
                    fn(peers_x[off_x], peers_y[off_y])

    small = (
        pltpu.make_async_copy(old_owner_hbm, old_owner, small_sem.at[0]),
        pltpu.make_async_copy(new_owner_hbm, new_owner, small_sem.at[1]),
        pltpu.make_async_copy(owner_row_hbm, owner_row, small_sem.at[2]),
        pltpu.make_async_copy(count_row, all_counts.at[me], small_sem.at[3]),
    )
    barrier = pltpu.get_barrier_semaphore()
    for off_y in offsets[:-1]:
        pl.semaphore_signal(barrier, inc=1, device_id=(gx, peers_y[off_y]), device_id_type=MESH)
    for off_x in range(1, groups_x):
        pl.semaphore_signal(barrier, inc=1, device_id=(peers_x[off_x], gy), device_id_type=MESH)

    for copy in small:
        copy.start()

    def old_piece(chunk, part):
        state, start, width = pieces[chunk]
        row = pl.multiple_of((part // splits) * SUBLANES, SUBLANES)
        col = pl.multiple_of((part % splits) * span + start, LANES)
        return olds[state].at[:, pl.ds(row, SUBLANES), pl.ds(col, width)]

    def own_rows(chunk):
        return by_rows[chunk].at[pl.ds(gx * held, held)]

    def local_copy(chunk, off):
        target = own_rows(chunk) if off == 0 else ready[chunk].at[off - 1]
        return pltpu.make_async_copy(old_piece(chunk, peers_x[off]), target, local_sem.at[chunk, off])

    def first_copy(chunk, off):
        return pltpu.make_async_remote_copy(
            src_ref=ready[chunk].at[off - 1],
            dst_ref=own_rows(chunk),
            send_sem=send1.at[chunk, off],
            recv_sem=recv1.at[chunk, off],
            device_id=(peers_x[off], gy),
            device_id_type=MESH,
        )

    order = range(chunks)
    for chunk in order:
        for off in [*range(1, groups_x), 0]:
            local_copy(chunk, off).start()

    pl.semaphore_wait(barrier, groups_x + groups_y - 2)
    for off_x in range(1, groups_x):
        pl.semaphore_signal(row_in, inc=1, device_id=(peers_x[off_x], gy), device_id_type=MESH)

    for chunk in order:
        for off in range(1, groups_x):
            local_copy(chunk, off).wait()
            first_copy(chunk, off).start()

    for copy in small:
        copy.wait()

    owners = [new_owner[e] for e in range(experts)]
    places = [old_owner[e] for e in range(experts)]

    def find(slot, carry):
        total = jnp.int32(0)
        for e in range(experts):
            total = total + jnp.where(owners[e] == slot, places[e], 0)
        source[slot] = total
        return carry

    lax.fori_loop(0, experts, find, 0)

    def count_copy(px, py):
        return pltpu.make_async_remote_copy(
            src_ref=count_row,
            dst_ref=all_counts.at[me],
            send_sem=send_c,
            recv_sem=recv_c,
            device_id=(px, py),
            device_id_type=MESH,
        )

    pl.semaphore_wait(row_in, groups_x - 1)
    def landing(chunk):
        state, start, width = pieces[chunk]
        row = pl.multiple_of(gy * rows + (gx // splits) * SUBLANES, SUBLANES)
        col = pl.multiple_of((gx % splits) * span + start, LANES)
        return outs[state].at[0, pl.ds(row, SUBLANES), pl.ds(col, width)]

    def self_copy(chunk):
        return pltpu.make_async_copy(staged[chunk].at[me], landing(chunk), self_sem.at[chunk])

    for chunk in order:
        local_copy(chunk, 0).wait()
        for off in range(1, groups_x):
            first_copy(chunk, off).wait_recv()

        def stage(slot, carry):
            staged[chunk][slot] = by_rows[chunk][source[slot]]
            return carry

        lax.fori_loop(0, experts, stage, 0, unroll=4)

        def send(px, py):
            pltpu.make_async_remote_copy(
                src_ref=staged[chunk].at[px * groups_y + py],
                dst_ref=landing(chunk),
                send_sem=send2.at[chunk],
                recv_sem=recv2.at[chunk],
                device_id=(px, py),
                device_id_type=MESH,
            ).start()

        for_peers(send)
        self_copy(chunk).start()
        if chunk == 0:
            for_peers(lambda px, py: count_copy(px, py).start())

    others = all_counts.at[pl.ds(0, devices - 1)]
    pltpu.make_async_copy(others, others, recv_c).wait()
    totals = jnp.sum(all_counts[...].astype(jnp.float32), axis=0)
    count = jnp.sum(jnp.where(owner_row[...] == me, totals, 0.0), axis=1, keepdims=True)
    count_out[...] = jnp.broadcast_to(count, count_out.shape)

    for chunk in order:
        for off in range(1, groups_x):
            first_copy(chunk, off).wait_send()
    pltpu.make_async_copy(others, others, send_c).wait()
    for chunk in order:
        self_copy(chunk).wait()
        sent = staged[chunk].at[pl.ds(0, devices - 1)]
        pltpu.make_async_copy(sent, sent, send2.at[chunk]).wait()
        pltpu.make_async_copy(sent, sent, recv2.at[chunk]).wait()


def tiled_plan(groups_x, groups_y, shape, experts):
    held, rows, cols = shape
    if rows % SUBLANES or experts != groups_x * groups_y:
        return None
    tiles = rows // SUBLANES
    if groups_x % tiles:
        return None
    span = cols // (groups_x // tiles)
    if span % LANES:
        return None
    half = (span // LANES + 1) // 2 * LANES
    pieces = [(state, 0, half) for state in range(3)]
    if half < span:
        pieces += [(state, half, span - half) for state in range(3)]
    if half > LANES:
        rest = [(state, LANES, half - LANES) for state in range(3)]
        pieces[:3] = [(state, 0, LANES) for state in range(3)] + rest
    return (groups_x, groups_y, experts, held, rows, tiles, span, tuple(pieces))


def kernel_body(dims, old_master, old_first, old_second, new_grad, counts, old_owner, new_owner):
    groups_x, groups_y, experts, held, rows, tiles, span, pieces = dims
    devices = groups_x * groups_y
    chunks = len(pieces)
    tile = (1, rows * groups_y, old_master.shape[2])
    vmem = pl.BlockSpec(memory_space=pltpu.VMEM)
    anywhere = pl.BlockSpec(memory_space=pl.ANY)
    buffers = [pltpu.VMEM((experts, SUBLANES, width), jnp.float32) for _, _, width in pieces] * 2
    buffers += [pltpu.VMEM((groups_x - 1, held, SUBLANES, width), jnp.float32) for _, _, width in pieces]
    row = new_owner.reshape(1, experts)
    operands = (old_owner, new_owner, row, counts.reshape(1, experts), old_master, old_first, old_second)
    kept = [pltpu.with_memory_space_constraint(array, pltpu.HBM) for array in operands]
    master, first, second, count = pl.pallas_call(
        functools.partial(rehome_kernel, dims),
        out_shape=[jax.ShapeDtypeStruct(tile, jnp.float32)] * 3 + [jax.ShapeDtypeStruct((1, LANES), jnp.float32)],
        in_specs=[pl.BlockSpec(memory_space=pltpu.HBM)] * 7,
        out_specs=[anywhere] * 3 + [vmem],
        scratch_shapes=buffers
        + [
            pltpu.SMEM((experts,), jnp.int32),
            pltpu.SMEM((experts,), jnp.int32),
            pltpu.SMEM((experts,), jnp.int32),
            pltpu.VMEM((1, experts), jnp.int32),
            pltpu.VMEM((devices, 1, experts), jnp.int32),
            pltpu.SemaphoreType.DMA((4,)),
            pltpu.SemaphoreType.DMA((chunks, groups_x)),
            pltpu.SemaphoreType.DMA((chunks,)),
            pltpu.SemaphoreType.DMA((chunks, groups_x)),
            pltpu.SemaphoreType.DMA((chunks, groups_x)),
            pltpu.SemaphoreType.DMA((chunks,)),
            pltpu.SemaphoreType.DMA((chunks,)),
            pltpu.SemaphoreType.DMA,
            pltpu.SemaphoreType.DMA,
            pltpu.SemaphoreType.REGULAR,
        ],
        compiler_params=pltpu.CompilerParams(collective_id=0, has_side_effects=True, vmem_limit_bytes=VMEM_GRANT),
    )(*kept)
    return adam_step(master, first, second, new_grad, count[0, 0])


def body(old_master, old_first, old_second, new_grad, counts, old_owner, new_owner):
    dims = tiled_plan(lax.axis_size("gx"), lax.axis_size("gy"), old_master.shape, old_owner.shape[0])
    if dims is None:
        return plain_body(old_master, old_first, old_second, new_grad, counts, old_owner, new_owner)
    return kernel_body(dims, old_master, old_first, old_second, new_grad, counts, old_owner, new_owner)


def solution(mesh):
    placed = (
        P("gx", "gy", None),
        P("gx", "gy", None),
        P("gx", "gy", None),
        P(("gx", "gy"), None, None),
        P(None, ("gx", "gy")),
        P(),
        P(),
    )
    return jax.shard_map(
        body,
        mesh=mesh,
        in_specs=placed,
        out_specs=(P(("gx", "gy"), None, None),) * 3,
        check_vma=False,
    )
```
